32 devices in a mesh: replica: 4 (over z), tensor: 8 (over y, x, core).
Axes of the slice: x: 2, y: 2, z: 4, core: 2. Of those that a mesh axis runs over, the one named last changes fastest.
Arguments:
- hidden_in: bfloat16 [4, 64, 8192], P(None, 'replica'), may hold values from -96 to 96
- norm_gain: bfloat16 [8192], replicated, may hold values from 0.25 to 1.75
- query_weight: bfloat16 [8192, 8192], P(None, 'tensor'), may hold values from -0.0625 to 0.0625
- w_keyvalue: bfloat16 [8192, 2048], P(None, 'tensor'), may hold values from -0.0625 to 0.0625
- output_weight: bfloat16 [8192, 8192], P('tensor'), may hold values from -0.0625 to 0.0625
- query_down_factor: bfloat16 [64, 8192], P(None, ('replica', 'tensor')), may hold values from -0.0625 to 0.0625
- query_up_factor: bfloat16 [64, 8192], P(None, ('replica', 'tensor')), may hold values from -0.75 to 0.75
- output_down_factor: bfloat16 [64, 8192], P(None, ('replica', 'tensor')), may hold values from -0.0625 to 0.0625
- output_up_factor: bfloat16 [64, 8192], P(None, ('replica', 'tensor')), may hold values from -0.75 to 0.75
- keys_cache: bfloat16 [16, 32, 1024, 128], P('tensor', 'replica'), may hold values from -250 to 250
- values_cache: bfloat16 [16, 32, 1024, 128], P('tensor', 'replica'), may hold values from -5 to 5
- cache_lengths: int32 [64], P('replica'), may hold values from 256 to 1024, as said below
Outputs:
- attended: bfloat16 [4, 64, 8192], P(None, 'replica', 'tensor')
The draws below stay inside these ranges and needn't reach their ends.
Inputs may be any that keep to these rules, and one draw needn't show every extreme that they name: `cache_lengths`: some row holds exactly 1024 positions and some other row exactly 256.
All inputs are finite; a program needn't handle non-finite values.
Results may differ from the reference program's by a relative error of at most 0.018.
Values may be sent and summed in bfloat16 or wider, within the bound.
No kernel may reach another device: no remote copies, remote signals or barrier semaphores. Data moves between devices by JAX's collectives and lax.ppermute only.
A program may use at most 128 MiB of HBM per device.

```python
import math
import jax
import jax.numpy as jnp
from jax import lax

D = 8192
HQ = 64
KVH = 8
HD = 128
RANK = 64
STEPS = 4
CAP = 1024
ROWS = 64


def draw_hidden_in(key, part):
    key_sample, key_rows, key_columns = jax.random.split(key, 3)
    sample = jax.random.normal(key_sample, (STEPS, ROWS, D), jnp.float32)
    row_scale = jnp.exp(jax.random.uniform(key_rows, (STEPS, ROWS, 1), jnp.float32, math.log(0.3), math.log(3.0)))
    column_scale = jnp.exp(jax.random.uniform(key_columns, (1, 1, D), jnp.float32, math.log(0.4), math.log(4.0)))
    return jnp.clip(sample * row_scale * column_scale, -96.0, 96.0).astype(jnp.bfloat16)


def draw_keys_cache(key, part):
    array_shape = (2 * KVH, ROWS // 2, CAP, HD)
    key_sample = jax.random.fold_in(key, 0)
    sample = jnp.clip(jax.random.normal(key_sample, array_shape, jnp.float32), -5.0, 5.0)
    return sample.astype(jnp.bfloat16)


def draw_cache_lengths(key, part):
    key_every, key_longest, key_shortest = jax.random.split(key, 3)
    lengths = jax.random.randint(key_every, (ROWS,), CAP // 4, CAP + 1)
    longest_row = jax.random.randint(key_longest, (), 0, ROWS)
    shortest_row = (longest_row + 1 + jax.random.randint(key_shortest, (), 0, ROWS - 1)) % ROWS
    row_numbers = jnp.arange(ROWS)
    lengths = jnp.where(row_numbers == longest_row, CAP, lengths)
    lengths = jnp.where(row_numbers == shortest_row, CAP // 4, lengths)
    return lengths.astype(jnp.int32)


def level_of(rng, shape, shards, low, top_value):
    gain, own = 1.0, jax.random.fold_in(rng, 6)
    for dim, parts in shards:
        steps = jnp.exp(jax.random.uniform(jax.random.fold_in(own, dim), (parts,), jnp.float32, low / len(shards), top_value / len(shards)))
        gain = gain * jnp.repeat(steps, shape[dim] // parts).reshape([-1 if axis == dim else 1 for axis in range(len(shape))])
    return gain


def normal_values(rng, dims, deviation, reach, shards=(), kind=jnp.bfloat16):
    entries = jax.random.normal(rng, dims, jnp.float32) * deviation
    if len(shards) > 0:
        entries = level_of(rng, dims, shards, -0.22, 0.18) * entries
    return jnp.clip(entries, min=-reach, max=reach).astype(kind)


def setup_inputs(seed: int = 0) -> dict:
    key_list = jax.random.split(jax.random.key(seed), 13)
    return {
        "hidden_in": draw_hidden_in(jax.random.fold_in(key_list[12], 71), 0),
        "norm_gain": jnp.clip(1.0 + 0.15 * jax.random.normal(key_list[1], (D,), jnp.float32), 0.25, 1.75).astype(jnp.bfloat16),
        "query_weight": normal_values(key_list[2], (D, HQ * HD), D ** -0.5, 0.0625, ((1, 8),)),
        "w_keyvalue": normal_values(key_list[3], (D, 2 * KVH * HD), D ** -0.5, 0.0625, ((1, 8),)),
        "output_weight": normal_values(key_list[4], (HQ * HD, D), (HQ * HD) ** -0.5, 0.0625, ((0, 8),)),
        "query_down_factor": normal_values(key_list[5], (RANK, D), D ** -0.5, 0.0625, ((1, 32),)),
        "query_up_factor": normal_values(key_list[6], (RANK, HQ * HD), RANK ** -0.5, 0.75, ((1, 32),)),
        "output_down_factor": normal_values(key_list[7], (RANK, HQ * HD), (HQ * HD) ** -0.5, 0.0625, ((1, 32),)),
        "output_up_factor": normal_values(key_list[8], (RANK, D), RANK ** -0.5, 0.75, ((1, 32),)),
        "keys_cache": draw_keys_cache(jax.random.fold_in(key_list[12], 71), 0),
        "values_cache": normal_values(key_list[10], (2 * KVH, ROWS // 2, CAP, HD), 1.0, 5.0, ((0, 8), (1, 4))),
        "cache_lengths": draw_cache_lengths(jax.random.fold_in(key_list[12], 71), 0),
    }


adapter_scale = 2.0
rope_base = 1000000.0
norm_epsilon = 1e-06

def rms_norm(hidden, norm_gain):
    values = hidden.astype(jnp.float32)
    mean_square = lax.optimization_barrier(jnp.mean(values * values, axis=-1, keepdims=True))
    return values * lax.rsqrt(mean_square + norm_epsilon) * norm_gain.astype(jnp.float32)

def apply_rotary(vectors, positions):
    half_width = vectors.shape[-1] // 2
    exponents = jnp.arange(half_width, dtype=jnp.float32) * (2.0 / vectors.shape[-1])
    frequency = jnp.power(rope_base, -exponents)
    angles = positions.astype(jnp.float32)[:, None, None] * frequency
    cosine_values = jnp.cos(angles)
    sine_values = jnp.sin(angles)
    leading = vectors[..., :half_width]
    trailing = vectors[..., half_width:]
    return jnp.concatenate([leading * cosine_values - trailing * sine_values, trailing * cosine_values + leading * sine_values], axis=-1)

def attend_block(queries, cache_keys, cache_values, lengths, fresh_keys, fresh_values):
    inverse_root = 1.0 / math.sqrt(queries.shape[-1])
    highest_precision = lax.Precision.HIGHEST
    query_float = queries.astype(jnp.float32)
    cached = jnp.einsum('ngd,npd->ngp', query_float, cache_keys.astype(jnp.float32), precision=highest_precision) * inverse_root
    visible = jnp.arange(cache_keys.shape[1])[None, :] < lengths[:, None]
    cached = jnp.where(visible[:, None, :], cached, -jnp.inf)
    recent = jnp.einsum('ngd,nsd->ngs', query_float, fresh_keys.astype(jnp.float32), precision=highest_precision) * inverse_root
    highest = jnp.maximum(lax.optimization_barrier(jnp.max(cached, axis=-1, keepdims=True)), lax.optimization_barrier(jnp.max(recent, axis=-1, keepdims=True)))
    cached_exp = jnp.exp(cached - highest)
    recent_exp = jnp.exp(recent - highest)
    denominator = lax.optimization_barrier(jnp.sum(cached_exp, axis=-1, keepdims=True)) + lax.optimization_barrier(jnp.sum(recent_exp, axis=-1, keepdims=True))
    cached_weight = (cached_exp / denominator).astype(jnp.bfloat16)
    recent_weight = (recent_exp / denominator).astype(jnp.bfloat16)
    combined = jnp.einsum('ngp,npd->ngd', cached_weight.astype(jnp.float32), cache_values.astype(jnp.float32), precision=highest_precision)
    combined = combined + jnp.einsum('ngs,nsd->ngd', recent_weight.astype(jnp.float32), fresh_values.astype(jnp.float32), precision=highest_precision)
    return combined.astype(jnp.bfloat16)

def reference(hidden_in, norm_gain, query_weight, w_keyvalue, output_weight, query_down_factor, query_up_factor, output_down_factor, output_up_factor, keys_cache, values_cache, cache_lengths):
    query_merged_weight = (query_weight.astype(jnp.float32) + adapter_scale * jnp.dot(query_down_factor.T, query_up_factor, preferred_element_type=jnp.float32)).astype(jnp.bfloat16)
    output_merged_weight = (output_weight.astype(jnp.float32) + adapter_scale * jnp.dot(output_down_factor.T, output_up_factor, preferred_element_type=jnp.float32)).astype(jnp.bfloat16)
    group_size = HQ // KVH
    keys_rows = keys_cache.reshape(KVH, 2, ROWS // 2, CAP, HD).transpose(0, 2, 1, 3, 4).reshape(KVH, ROWS, CAP, HD)
    values_rows = values_cache.reshape(KVH, 2, ROWS // 2, CAP, HD).transpose(0, 2, 1, 3, 4).reshape(KVH, ROWS, CAP, HD)
    fresh_key_list = []
    fresh_value_list = []
    results = []
    for decode_step in range(STEPS):
        normed = rms_norm(hidden_in[decode_step], norm_gain).astype(jnp.bfloat16)
        positions = cache_lengths + decode_step
        queries = jnp.dot(normed, query_merged_weight, preferred_element_type=jnp.float32).reshape(ROWS, HQ, HD)
        queries = apply_rotary(queries, positions).astype(jnp.bfloat16)
        keyvals = jnp.dot(normed, w_keyvalue, preferred_element_type=jnp.float32).reshape(ROWS, KVH, 2, HD)
        fresh_key_list.append(apply_rotary(keyvals[:, :, 0], positions).astype(jnp.bfloat16))
        fresh_value_list.append(keyvals[:, :, 1].astype(jnp.bfloat16))
        stacked_keys = jnp.stack(fresh_key_list, axis=1)
        stacked_values = jnp.stack(fresh_value_list, axis=1)
        outputs = []
        for group_index in range(KVH):
            outputs.append(attend_block(queries[:, group_index * group_size:(group_index + 1) * group_size], keys_rows[group_index], values_rows[group_index], cache_lengths, stacked_keys[:, :, group_index], stacked_values[:, :, group_index]))
        heads_all = jnp.concatenate(outputs, axis=1).reshape(ROWS, HQ * HD)
        results.append(jnp.dot(heads_all, output_merged_weight, preferred_element_type=jnp.float32).astype(jnp.bfloat16))
    return jnp.stack(results)
```

```python
import math

import jax
import jax.numpy as jnp
import numpy as np
from jax import lax
from jax.experimental import pallas as pl
from jax.experimental.pallas import tpu as pltpu
from jax.sharding import PartitionSpec as P

HQ = 64
KVH = 8
HD = 128
CAP = 1024


adapter_scale = 2.0
rope_base = 1000000.0
norm_epsilon = 1e-06


def swapped(array, axis, apart):
    return lax.ppermute(array, axis, [(i, i ^ 1 << apart) for i in range(lax.axis_size(axis))])


def for_sending(array):
    return jax.tree.map(lambda a: a.astype(jnp.bfloat16) if a.dtype == jnp.float32 else a, array)


def rms_norm(hidden, norm_gain):
    values = hidden.astype(jnp.float32)
    mean_square = jnp.mean(values * values, axis=-1, keepdims=True)
    return values * lax.rsqrt(mean_square + norm_epsilon) * norm_gain.astype(jnp.float32)


def apply_rotary(vectors, positions):
    half_width = vectors.shape[-1] // 2
    exponents = jnp.arange(half_width, dtype=jnp.float32) * (2.0 / vectors.shape[-1])
    frequency = jnp.power(rope_base, -exponents)
    angles = positions.astype(jnp.float32)[:, None, None] * frequency
    cosine_values = jnp.cos(angles)
    sine_values = jnp.sin(angles)
    leading = vectors[..., :half_width]
    trailing = vectors[..., half_width:]
    return jnp.concatenate(
        [
            leading * cosine_values - trailing * sine_values,
            trailing * cosine_values + leading * sine_values,
        ],
        axis=-1,
    )


def attend_block(queries, cache_keys, cache_values, lengths, fresh_keys, fresh_values):
    inverse_root = 1.0 / math.sqrt(queries.shape[-1])
    cached = (
        jnp.einsum("ngd,npd->ngp", queries, cache_keys, preferred_element_type=jnp.float32)
        * inverse_root
    )
    visible = jnp.arange(cache_keys.shape[1])[None, :] < lengths[:, None]
    cached = jnp.where(visible[:, None, :], cached, -jnp.inf)
    recent = (
        jnp.einsum("ngd,nsd->ngs", queries, fresh_keys, preferred_element_type=jnp.float32)
        * inverse_root
    )
    highest = jnp.maximum(
        jnp.max(cached, axis=-1, keepdims=True), jnp.max(recent, axis=-1, keepdims=True)
    )
    cached_exp = jnp.exp(cached - highest)
    recent_exp = jnp.exp(recent - highest)
    denominator = jnp.sum(cached_exp, axis=-1, keepdims=True) + jnp.sum(
        recent_exp, axis=-1, keepdims=True
    )
    cached_weight = (cached_exp / denominator).astype(jnp.bfloat16)
    recent_weight = (recent_exp / denominator).astype(jnp.bfloat16)
    combined = jnp.einsum(
        "ngp,npd->ngd", cached_weight, cache_values, preferred_element_type=jnp.float32
    )
    combined = combined + jnp.einsum(
        "ngs,nsd->ngd", recent_weight, fresh_values, preferred_element_type=jnp.float32
    )
    return combined.astype(jnp.bfloat16)


def rank_contraction(left_factor, right_factor):
    return lax.dot_general(
        left_factor, right_factor, (((0,), (0,)), ((), ())), preferred_element_type=jnp.float32
    )


def pick_half(paired, lower_half):
    return jnp.where(lower_half, paired[:, 0], paired[:, 1])


def pick_middle(paired, lower_half):
    return jnp.where(lower_half, paired[:, :, 0], paired[:, :, 1])


def shards(
    hidden_in,
    norm_gain,
    query_weight,
    w_keyvalue,
    output_weight,
    query_down_factor,
    query_up_factor,
    output_down_factor,
    output_up_factor,
    keys_cache,
    values_cache,
    cache_lengths,
):
    tensor_index = lax.axis_index("tensor")
    slice_width = query_weight.shape[1]
    complete_down_factor, complete_up_factor, wide_up, wide_down = (
        lax.all_gather(query_down_factor, ("replica", "tensor"), axis=1, tiled=True),
        lax.all_gather(output_up_factor, ("replica", "tensor"), axis=1, tiled=True),
        lax.all_gather(query_up_factor, ("replica", "tensor"), axis=1, tiled=True),
        lax.all_gather(output_down_factor, ("replica", "tensor"), axis=1, tiled=True),
    )
    query_weight_slice = lax.dynamic_slice_in_dim(
        wide_up, tensor_index * slice_width, slice_width, 1
    )
    output_weight_slice = lax.dynamic_slice_in_dim(
        wide_down, tensor_index * slice_width, slice_width, 1
    )
    query_merged_weight = (
        query_weight.astype(jnp.float32)
        + adapter_scale * rank_contraction(complete_down_factor, query_weight_slice)
    ).astype(jnp.bfloat16)
    output_merged_weight = (
        output_weight.astype(jnp.float32)
        + adapter_scale * rank_contraction(output_weight_slice, complete_up_factor)
    ).astype(jnp.bfloat16)
    rows_local = hidden_in.shape[1]
    rows_half = rows_local // 2
    heads_local = slice_width // HD
    group_size = HQ // KVH
    entries = keys_cache.shape[0]
    lower_half = tensor_index % 2 == 0
    groups_local = max(heads_local // group_size, 1)
    block_count = groups_local * 2 * rows_half
    if entries == 1:
        own_lengths = pick_half(cache_lengths.reshape(rows_half, 2), lower_half)
        own_keys = keys_cache[0]
        own_values = values_cache[0]
    else:
        own_lengths = jnp.tile(cache_lengths.reshape(rows_half, 2).T, (groups_local, 1)).reshape(
            block_count
        )
        own_keys = keys_cache.reshape(block_count, CAP, HD)
        own_values = values_cache.reshape(block_count, CAP, HD)
    step_count = hidden_in.shape[0]
    normed_all = (
        rms_norm(hidden_in, norm_gain)
        .astype(jnp.bfloat16)
        .reshape(step_count * rows_local, hidden_in.shape[2])
    )
    positions_all = (
        cache_lengths[None, :] + jnp.arange(step_count, dtype=jnp.int32)[:, None]
    ).reshape(step_count * rows_local)
    queries_all = jnp.dot(
        normed_all, query_merged_weight, preferred_element_type=jnp.float32
    ).reshape(step_count * rows_local, heads_local, HD)
    queries_all = apply_rotary(queries_all, positions_all).astype(jnp.bfloat16)
    projected_all = jnp.dot(normed_all, w_keyvalue, preferred_element_type=jnp.float32)
    heads_list = []
    if entries == 1:
        rotated_all = apply_rotary(projected_all[:, None, :], positions_all)[:, 0]
        projected_all = jnp.where(lower_half, rotated_all, projected_all).astype(jnp.bfloat16)
        query_pairs = queries_all.reshape(step_count, rows_half, 2, heads_local, HD)
        projected_pairs = projected_all.reshape(step_count, rows_half, 2, HD)
        own_queries = pick_middle(query_pairs, lower_half)
        other_queries = pick_middle(query_pairs, jnp.logical_not(lower_half))
        own_projected = pick_middle(projected_pairs, lower_half)
        other_projected = pick_middle(projected_pairs, jnp.logical_not(lower_half))
        outgoing = jnp.concatenate(
            [other_queries.reshape(step_count, rows_half, heads_local * HD), other_projected],
            axis=2,
        )
        incoming = swapped(outgoing, "tensor", 0)
        partner_queries = incoming[:, :, : heads_local * HD].reshape(
            step_count, rows_half, heads_local, HD
        )
        partner_projected = incoming[:, :, heads_local * HD :]
        group_queries_all = jnp.where(
            lower_half,
            jnp.concatenate([own_queries, partner_queries], axis=2),
            jnp.concatenate([partner_queries, own_queries], axis=2),
        )
        keys_steps = jnp.where(lower_half, own_projected, partner_projected).transpose(1, 0, 2)
        values_steps = jnp.where(lower_half, partner_projected, own_projected).transpose(1, 0, 2)
        kept_list = []
        sent_list = []
        for decode_step in range(step_count):
            attended_heads = attend_block(
                group_queries_all[decode_step],
                own_keys,
                own_values,
                own_lengths,
                keys_steps[:, : decode_step + 1],
                values_steps[:, : decode_step + 1],
            )
            first_heads = attended_heads[:, :heads_local]
            second_heads = attended_heads[:, heads_local:]
            kept_list.append(
                jnp.where(lower_half, first_heads, second_heads).reshape(
                    rows_half, heads_local * HD
                )
            )
            sent_list.append(
                jnp.where(lower_half, second_heads, first_heads).reshape(
                    rows_half, heads_local * HD
                )
            )
        kept_all = jnp.stack(kept_list)
        returned_all = swapped(for_sending(jnp.stack(sent_list)), "tensor", 0)
        rows_first = jnp.where(lower_half, kept_all, returned_all)
        rows_second = jnp.where(lower_half, returned_all, kept_all)
        heads_stacked = jnp.stack([rows_first, rows_second], axis=2).reshape(
            step_count * rows_local, heads_local * HD
        )
    else:
        keyvals = projected_all.reshape(step_count, rows_local, groups_local, 2, HD)
        new_keys = apply_rotary(
            keyvals[:, :, :, 0].reshape(step_count * rows_local, groups_local, HD), positions_all
        ).astype(jnp.bfloat16)
        new_values = keyvals[:, :, :, 1].astype(jnp.bfloat16)
        keys_steps = (
            new_keys.reshape(step_count, rows_half, 2, groups_local, HD)
            .transpose(3, 2, 1, 0, 4)
            .reshape(block_count, step_count, HD)
        )
        values_steps = (
            new_values.reshape(step_count, rows_half, 2, groups_local, HD)
            .transpose(3, 2, 1, 0, 4)
            .reshape(block_count, step_count, HD)
        )
        group_queries_all = (
            queries_all.reshape(step_count, rows_half, 2, groups_local, group_size, HD)
            .transpose(0, 3, 2, 1, 4, 5)
            .reshape(step_count, block_count, group_size, HD)
        )
        for decode_step in range(step_count):
            attended_heads = attend_block(
                group_queries_all[decode_step],
                own_keys,
                own_values,
                own_lengths,
                keys_steps[:, : decode_step + 1],
                values_steps[:, : decode_step + 1],
            )
            heads_list.append(
                attended_heads.reshape(groups_local, 2, rows_half, group_size, HD)
                .transpose(2, 1, 0, 3, 4)
                .reshape(rows_local, heads_local * HD)
            )
        heads_stacked = jnp.stack(heads_list).reshape(step_count * rows_local, heads_local * HD)
    partial_all = jnp.dot(heads_stacked, output_merged_weight, preferred_element_type=jnp.float32)
    shares_all = lax.psum_scatter(
        partial_all.astype(jnp.bfloat16), "tensor", scatter_dimension=1, tiled=True
    ).astype(jnp.float32)
    return shares_all.reshape(step_count, rows_local, shares_all.shape[1]).astype(jnp.bfloat16)


MIB = 1 << 20
PROJECT_CHUNKS = 8


def dot32(left, right):
    return jnp.dot(left, right, preferred_element_type=jnp.float32)


def dot_nt(left, right):
    return lax.dot_general(
        left, right, (((1,), (1,)), ((), ())), preferred_element_type=jnp.float32
    )


def rotate(vectors, cosines, sines):
    return vectors * cosines + pltpu.roll(vectors, vectors.shape[-1] // 2, 1) * sines


def project_kernel(
    lengths_ref,
    hidden_ref,
    gain_ref,
    frequency_ref,
    wq_hbm,
    wkv_hbm,
    query_ref,
    key_ref,
    value_ref,
    normed_ref,
    cosine_ref,
    sine_ref,
    wq_buf,
    wkv_buf,
    acc_kv,
    q_sems,
    kv_sems,
):
    rows, width = hidden_ref.shape
    rows_local = lengths_ref.shape[0]
    chunk = width // PROJECT_CHUNKS

    def copies(i):
        at = pl.ds(i * chunk, chunk)
        return (
            pltpu.make_async_copy(wq_hbm.at[at], wq_buf.at[at], q_sems.at[i]),
            pltpu.make_async_copy(wkv_hbm.at[at], wkv_buf.at[at], kv_sems.at[i]),
        )

    for i in range(PROJECT_CHUNKS):
        for copy in copies(i):
            copy.start()
    square = jnp.zeros((rows, 128), jnp.float32)
    for i in range(PROJECT_CHUNKS):
        piece = hidden_ref[:, i * chunk : (i + 1) * chunk].astype(jnp.float32)
        piece = piece * piece
        for j in range(chunk // 128):
            square = square + piece[:, j * 128 : (j + 1) * 128]
    scale = lax.rsqrt(jnp.sum(square, axis=1, keepdims=True) / width + norm_epsilon)
    for i in range(PROJECT_CHUNKS):
        at = slice(i * chunk, (i + 1) * chunk)
        piece = hidden_ref[:, at].astype(jnp.float32) * scale
        normed_ref[:, at] = (piece * gain_ref[:, at].astype(jnp.float32)).astype(jnp.bfloat16)
    row = lax.broadcasted_iota(jnp.int32, (rows, HD), 0)
    position = row // rows_local
    for b in range(rows_local):
        position = position + jnp.where(row % rows_local == b, lengths_ref[b], 0)
    angle = position.astype(jnp.float32) * frequency_ref[...]
    lane = lax.broadcasted_iota(jnp.int32, (rows, HD), 1)
    cosines = jnp.cos(angle)
    sines = jnp.where(lane < HD // 2, -jnp.sin(angle), jnp.sin(angle))
    cosine_ref[...] = cosines
    sine_ref[...] = sines
    for i in range(PROJECT_CHUNKS):
        at = slice(i * chunk, (i + 1) * chunk)
        for copy in copies(i):
            copy.wait()
        part = normed_ref[:, at]
        q_part = dot32(part, wq_buf[at])
        kv_part = dot32(part, wkv_buf[at])
        if i == 0:
            query_ref[...] = q_part
            acc_kv[...] = kv_part
        else:
            query_ref[...] += q_part
            acc_kv[...] += kv_part
    key_ref[...] = rotate(acc_kv[:, :HD], cosines, sines)
    value_ref[...] = acc_kv[:, HD:]


def low_rank_kernel(blocks, normed_ref, *refs):
    factors, out_ref = refs[:-1], refs[-1]
    replica, tensor = lax.axis_index("replica"), lax.axis_index("tensor")
    tensor_size = normed_ref.shape[1] // (factors[0].shape[1] * blocks)
    wide = factors[0].shape[1]
    total = None
    for p, factor in enumerate(factors):
        at = pl.multiple_of(((replica ^ p) * tensor_size + tensor) * wide, wide)
        part = dot_nt(normed_ref[:, pl.ds(at, wide)], factor[...])
        total = part if total is None else total + part
    out_ref[...] = total


def attend_kernel(
    steps,
    lengths_ref,
    query_ref,
    low0_ref,
    low1_ref,
    low2_ref,
    low3_ref,
    factors_ref,
    key_ref,
    value_ref,
    cosine_ref,
    sine_ref,
    keys_ref,
    values_ref,
    wo_hbm,
    half_ref,
    low_out_ref,
    send_ref,
    heads_ref,
    q_rows,
    o_rows,
    fresh_keys,
    fresh_values,
    q_full,
    wo_buf,
    wo_sems,
):
    replica, tensor = lax.axis_index("replica"), lax.axis_index("tensor")
    rows, width = query_ref.shape
    quarters = wo_hbm.shape[1] // (2 * width)
    mine = tensor % 2

    def weight_copy(i):
        at = (2 * (i % quarters) + (1 - mine if i < quarters else mine)) * width
        source = wo_hbm.at[:, pl.ds(pl.multiple_of(at, width), width)]
        return pltpu.make_async_copy(source, wo_buf.at[i], wo_sems.at[i])

    for i in range(2 * quarters):
        weight_copy(i).start()
    rows_local = rows // steps
    group = width // HD
    per_row = steps * group
    blocks, _, wide = factors_ref.shape
    rank = low0_ref.shape[1]
    low = (low0_ref[...] + low1_ref[...]) + (low2_ref[...] + low3_ref[...])
    low = (low * adapter_scale).astype(jnp.bfloat16)
    for p in range(blocks):
        at = pl.ds(pl.multiple_of((replica ^ p) * wide, wide), wide)
        q_full[:, at] = query_ref[:, at] + dot32(low, factors_ref[p, :rank, :])
    cosines, sines = cosine_ref[...], sine_ref[...]
    for h in range(group):
        turned = rotate(q_full[:, h * HD : (h + 1) * HD], cosines, sines)
        for t in range(steps):
            q_rows[pl.ds(t * group + h, rows_local, stride=per_row), :] = turned[
                t * rows_local : (t + 1) * rows_local
            ]
    pad = fresh_keys.shape[0] // rows_local
    fresh_keys[...] = jnp.zeros_like(fresh_keys)
    fresh_values[...] = jnp.zeros_like(fresh_values)
    for t in range(steps):
        at = slice(t * rows_local, (t + 1) * rows_local)
        fresh_keys[pl.ds(t, rows_local, stride=pad), :] = key_ref[at]
        fresh_values[pl.ds(t, rows_local, stride=pad), :] = value_ref[at]
    new_keys = fresh_keys[...].astype(jnp.bfloat16)
    new_values = fresh_values[...].astype(jnp.bfloat16)
    inverse_root = 1.0 / math.sqrt(HD)
    capacity = keys_ref.shape[2]
    place = lax.broadcasted_iota(jnp.int32, (per_row, capacity), 1)
    fresh_place = lax.broadcasted_iota(jnp.int32, (per_row, fresh_keys.shape[0]), 1)
    fresh_step = lax.broadcasted_iota(jnp.int32, (per_row, fresh_keys.shape[0]), 0) // group
    for b in range(rows_local):
        queries = q_rows[b * per_row : (b + 1) * per_row].astype(jnp.bfloat16)
        cached = dot_nt(queries, keys_ref[b % 2, b // 2]) * inverse_root
        cached = jnp.where(place < lengths_ref[b], cached, -jnp.inf)
        fresh = dot_nt(queries, new_keys) * inverse_root
        offset = fresh_place - b * pad
        seen = jnp.logical_and(offset >= 0, offset <= fresh_step)
        fresh = jnp.where(seen, fresh, -jnp.inf)
        highest = jnp.maximum(
            jnp.max(cached, axis=1, keepdims=True), jnp.max(fresh, axis=1, keepdims=True)
        )
        cached = jnp.exp(cached - highest)
        fresh = jnp.exp(fresh - highest)
        total = jnp.sum(cached, axis=1, keepdims=True) + jnp.sum(fresh, axis=1, keepdims=True)
        mixed = dot32(cached.astype(jnp.bfloat16), values_ref[b % 2, b // 2]) + dot32(
            fresh.astype(jnp.bfloat16), new_values
        )
        o_rows[b * per_row : (b + 1) * per_row] = mixed / total
    for h in range(group):
        for t in range(steps):
            heads_ref[t * rows_local : (t + 1) * rows_local, h * HD : (h + 1) * HD] = o_rows[
                pl.ds(t * group + h, rows_local, stride=per_row), :
            ].astype(jnp.bfloat16)
    low_out = None
    for p in range(blocks):
        at = pl.ds(pl.multiple_of((replica ^ p) * wide, wide), wide)
        part = dot_nt(heads_ref[:, at], factors_ref[p, rank : 2 * rank, :])
        low_out = part if low_out is None else low_out + part
    low_out_ref[...] = low_out
    heads = heads_ref[...]
    for q in range(quarters):
        weight_copy(q).wait()
        send_ref[:, q * width : (q + 1) * width] = dot32(heads, wo_buf[q]).astype(jnp.bfloat16)
    high = low_out.astype(jnp.bfloat16)
    rest = (low_out - high.astype(jnp.float32)).astype(jnp.bfloat16)
    send_ref[:, quarters * width :] = jnp.concatenate([high, rest], axis=1)
    for q in range(quarters):
        weight_copy(quarters + q).wait()
        half_ref[q] = dot32(heads, wo_buf[quarters + q])


def split_kernel(half_ref, low_ref, received_ref, kept_ref, *send_refs):
    tensor = lax.axis_index("tensor")
    quarters, rows, width = half_ref.shape
    rank = low_ref.shape[1]
    own = tensor // 2
    extra = received_ref[:, quarters * width :].astype(jnp.float32)
    low = low_ref[...] + extra[:, :rank] + extra[:, rank:]
    high = low.astype(jnp.bfloat16)
    rest = (low - high.astype(jnp.float32)).astype(jnp.bfloat16)
    tail = jnp.concatenate([high, rest], axis=1)
    for k in range(quarters):
        q = own ^ k
        at = pl.ds(pl.multiple_of(q * width, width), width)
        total = half_ref[q] + received_ref[:, at].astype(jnp.float32)
        if k == 0:
            kept_ref[:, :width] = total
            kept_ref[:, width:] = jnp.concatenate([low, jnp.zeros_like(low)], axis=1)
        else:
            send_refs[k - 1][:, :width] = total.astype(jnp.bfloat16)
            send_refs[k - 1][:, width:] = tail


def finish_kernel(kept_ref, factors_ref, *refs):
    received, out_ref = refs[:-1], refs[-1]
    replica = lax.axis_index("replica")
    blocks, rank3, wide = factors_ref.shape
    rank = rank3 // 3
    width = blocks * wide
    extra = kept_ref[:, width:]
    for r in received:
        extra = extra + r[:, width:].astype(jnp.float32)
    low = ((extra[:, :rank] + extra[:, rank:]) * adapter_scale).astype(jnp.bfloat16)
    for p in range(blocks):
        at = pl.ds(pl.multiple_of((replica ^ p) * wide, wide), wide)
        total = kept_ref[:, at] + dot32(low, factors_ref[p, 2 * rank :, :])
        for r in received:
            total = total + r[:, at].astype(jnp.float32)
        out_ref[:, at] = total.astype(jnp.bfloat16)


def vmem():
    return pl.BlockSpec(memory_space=pltpu.VMEM)


def smem():
    return pl.BlockSpec(memory_space=pltpu.SMEM)


def hbm():
    return pl.BlockSpec(memory_space=pltpu.HBM)


def shape_of(shape, dtype):
    return jax.ShapeDtypeStruct(shape, dtype)


def params(mib):
    return pltpu.CompilerParams(vmem_limit_bytes=mib * MIB)


def in_vmem(array):
    return pltpu.with_memory_space_constraint(array, pltpu.VMEM)


def in_hbm(array):
    return pltpu.with_memory_space_constraint(array, pltpu.HBM)


def fast_shards(
    hidden_in,
    norm_gain,
    query_weight,
    w_keyvalue,
    output_weight,
    query_down_factor,
    query_up_factor,
    output_down_factor,
    output_up_factor,
    keys_cache,
    values_cache,
    cache_lengths,
):
    replicas, tensors = lax.axis_size("replica"), lax.axis_size("tensor")
    steps, rows_local, model = hidden_in.shape
    rows = steps * rows_local
    width = query_weight.shape[1]
    rank, wide = query_down_factor.shape
    f32, bf16 = jnp.float32, jnp.bfloat16

    def over_replica(array, k):
        return lax.ppermute(array, "replica", [(i, i ^ k) for i in range(replicas)])

    def over_tensor(array, k):
        return lax.ppermute(array, "tensor", [(i, i ^ k) for i in range(tensors)])

    down = [query_down_factor] + [over_replica(query_down_factor, k) for k in range(1, replicas)]
    others = jnp.concatenate([query_up_factor, output_down_factor, output_up_factor], axis=0)
    gathered = jnp.stack([others] + [over_tensor(others, k) for k in range(1, replicas)])
    groups = tensors // replicas
    home = [
        (z * tensors + t, (t % replicas) * tensors + z * groups + t // replicas)
        for z in range(replicas)
        for t in range(tensors)
    ]
    factors = lax.ppermute(gathered, ("replica", "tensor"), home)

    exponents = np.arange(HD // 2, dtype=np.float32) * np.float32(2.0 / HD)
    frequency = np.power(rope_base, -exponents.astype(np.float64)).astype(np.float32)
    frequency = jnp.asarray(np.concatenate([frequency, frequency])[None])
    chunk_sems = pltpu.SemaphoreType.DMA((PROJECT_CHUNKS,))
    query, key, value, normed, cosines, sines = pl.pallas_call(
        project_kernel,
        name="project",
        out_shape=(
            shape_of((rows, width), f32),
            shape_of((rows, HD), f32),
            shape_of((rows, HD), f32),
            shape_of((rows, model), bf16),
            shape_of((rows, HD), f32),
            shape_of((rows, HD), f32),
        ),
        in_specs=[smem(), vmem(), vmem(), vmem(), hbm(), hbm()],
        out_specs=(vmem(),) * 6,
        scratch_shapes=[
            pltpu.VMEM(query_weight.shape, bf16),
            pltpu.VMEM(w_keyvalue.shape, bf16),
            pltpu.VMEM((rows, 2 * HD), f32),
            chunk_sems,
            chunk_sems,
        ],
        compiler_params=params(28),
    )(
        cache_lengths,
        hidden_in.reshape(rows, model),
        norm_gain[None],
        frequency,
        in_hbm(query_weight),
        in_hbm(w_keyvalue),
    )
    low = pl.pallas_call(
        lambda *refs: low_rank_kernel(replicas, *refs),
        name="low_rank",
        out_shape=shape_of((rows, rank), f32),
        in_specs=[vmem()] * (1 + replicas),
        out_specs=vmem(),
        compiler_params=params(8),
    )(normed, *down)
    low = low + over_tensor(low, 1)
    lows = [low] + [over_tensor(low, 2 * k) for k in range(1, tensors // 2)]

    per_row = steps * (width // HD)
    half, low_out, sent = pl.pallas_call(
        lambda *refs: attend_kernel(steps, *refs),
        name="attend",
        out_shape=(
            shape_of((tensors // 2, rows, width), f32),
            shape_of((rows, rank), f32),
            shape_of((rows, model // 2 + 2 * rank), bf16),
        ),
        in_specs=[smem()] + [vmem()] * 12 + [hbm()],
        out_specs=(vmem(),) * 3,
        scratch_shapes=[
            pltpu.VMEM((rows, width), bf16),
            pltpu.VMEM((rows_local * per_row, HD), f32),
            pltpu.VMEM((rows_local * per_row, HD), f32),
            pltpu.VMEM((rows_local * 8, HD), f32),
            pltpu.VMEM((rows_local * 8, HD), f32),
            pltpu.VMEM((rows, width), f32),
            pltpu.VMEM((tensors, width, width), bf16),
            pltpu.SemaphoreType.DMA((tensors,)),
        ],
        compiler_params=params(34),
    )(
        cache_lengths,
        query,
        *lows,
        factors,
        key,
        value,
        cosines,
        sines,
        in_vmem(keys_cache),
        in_vmem(values_cache),
        in_hbm(output_weight),
    )
    received = over_tensor(sent, 1)
    kept, *sends = pl.pallas_call(
        split_kernel,
        name="split",
        out_shape=(
            shape_of((rows, width + 2 * rank), f32),
            *[shape_of((rows, width + 2 * rank), bf16)] * (tensors // 2 - 1),
        ),
        in_specs=[vmem()] * 3,
        out_specs=(vmem(),) * (tensors // 2),
        compiler_params=params(16),
    )(half, low_out, received)
    returned = [over_tensor(s, 2 * (k + 1)) for k, s in enumerate(sends)]
    out = pl.pallas_call(
        finish_kernel,
        name="finish",
        out_shape=shape_of((rows, width), bf16),
        in_specs=[vmem()] * (2 + len(returned)),
        out_specs=vmem(),
        compiler_params=params(16),
    )(kept, factors, *returned)
    return out.reshape(steps, rows_local, width)


def power_of_two(number):
    return number & (number - 1) == 0


def any_shards(*arrays):
    replicas, tensors = lax.axis_size("replica"), lax.axis_size("tensor")
    hidden_in, query_weight, keys_cache = arrays[0], arrays[2], arrays[9]
    fits = (
        power_of_two(replicas)
        and power_of_two(tensors)
        and tensors == 8
        and tensors % replicas == 0
        and keys_cache.shape[0] == 2
        and query_weight.shape[1] == (HQ // KVH) * HD
        and hidden_in.shape[1] % 8 == 0
        and hidden_in.shape[0] <= 8
    )
    return fast_shards(*arrays) if fits else shards(*arrays)


def solution(mesh):
    return jax.shard_map(
        any_shards,
        mesh=mesh,
        in_specs=(
            P(None, "replica", None),
            P(),
            P(None, "tensor"),
            P(None, "tensor"),
            P("tensor", None),
            P(None, ("replica", "tensor")),
            P(None, ("replica", "tensor")),
            P(None, ("replica", "tensor")),
            P(None, ("replica", "tensor")),
            P("tensor", "replica", None, None),
            P("tensor", "replica", None, None),
            P("replica"),
        ),
        out_specs=P(None, "replica", "tensor"),
        check_vma=False,
    )
```
